32 devices in a mesh: rep: 2 (over x), shard: 16 (over z, y, core).
Axes of the slice: x: 2, y: 2, z: 4, core: 2. Of those that a mesh axis runs over, the one named last changes fastest.
Arguments:
- hidden: bfloat16 [12288, 64], P(('rep', 'shard')), may hold values from -6 to 6
- grad_out: bfloat16 [12288, 4096], P(('rep', 'shard')), may hold values from -6 to 6
- weight_band: bfloat16 [64, 4096], P('shard'), may hold values from -0.09375 to 0.09375
- error_feedback: float32 [2, 64, 4096], P('rep', 'shard'), may hold values from -4.2426405 to 4.2426405
- q_start: float32 [4096, 32], replicated, may hold values from -6 to 6
Outputs:
- update: float32 [64, 4096], P('shard')
- error_next: float32 [2, 64, 4096], P('rep', 'shard')
- q_next: float32 [4096, 32], replicated
- d_hidden: bfloat16 [12288, 64], P(('rep', 'shard'))
The draws below stay inside these ranges and needn't reach their ends.
All inputs are finite; a program needn't handle non-finite values.
Results may differ from the reference program's by a relative error of at most 0.0004.
Values may be sent and summed in bfloat16 or wider, within the bound.
A program may use at most 64 MiB of HBM per device.

```python
import math
import jax
import jax.numpy as jnp
from jax import lax

D = 4096
TOK_DEV = 384
RANK = 32
POWER = 2
BUCKET = 64
TOKENS = 12288
N_REP = 2
N_SHARD = 16


def spiked(result, key, source, target, blocks, factor):
    owner, partner = [(jnp.arange(result.shape[dim]) // (result.shape[dim] // blocks)).reshape([-1 if axis == dim else 1 for axis in range(result.ndim)]) for dim in (source, target)]
    chosen = jax.random.permutation(key, blocks)[partner]
    strong = (owner == chosen) | (owner == (partner + blocks // 2) % blocks)
    return jnp.where(strong, factor * result, result)


def block_scale(key, shape, pieces, low, top_value):
    def one(axis_at, parts):
        steps = jax.random.uniform(jax.random.fold_in(jax.random.fold_in(key, 6), axis_at), (parts,), jnp.float32, low / len(pieces), top_value / len(pieces))
        return jnp.repeat(jnp.exp(steps), shape[axis_at] // parts).reshape((-1,) + (1,) * (len(shape) - axis_at - 1))

    gain = one(*pieces[0])
    for cut in pieces[1:]:
        gain = gain * one(*cut)
    return gain


def centred(key, dims, scale, reach, cuts=(), dtype=jnp.bfloat16):
    result = jax.random.normal(key, dims, jnp.float32) * scale
    if len(cuts) > 0:
        result = block_scale(key, dims, cuts, -0.22, 0.18) * result
    return jnp.clip(result, min=-reach, max=reach).astype(dtype)


def noise_with(key, shape, deviation, bound, cuts, heavy, dtype=jnp.bfloat16):
    array = deviation * jax.random.normal(key, shape, jnp.float32)
    if cuts:
        array = array * block_scale(key, shape, cuts, -0.22, 0.18)
    return jnp.clip(spiked(array, jax.random.fold_in(key, 3), *heavy), -bound, bound).astype(dtype)


def setup_inputs(seed: int = 0) -> dict:
    key_of = jax.random.split(jax.random.key(seed), 6)
    hidden = noise_with(key_of[0], (TOKENS, BUCKET), 1.0, 6.0, ((0, 32),), (0, 1, 32, 2.75))
    grad_out = centred(key_of[1], (TOKENS, D), 1.0, 6.0, ((0, 32),))
    weight_band = centred(key_of[2], (BUCKET, D), D ** -0.5, 0.09375, ((0, 16),))
    error_feedback = centred(key_of[3], (N_REP, BUCKET, D), (1.0 / N_REP ** 0.5), 4.2426405, ((0, 2), (1, 16)), jnp.float32)
    q_start = centred(key_of[4], (D, RANK), 1.0, 6.0, (), jnp.float32)
    return dict(hidden=hidden, grad_out=grad_out, weight_band=weight_band, error_feedback=error_feedback, q_start=q_start)


def orthonormal(matrix):
    gram_matrix = jnp.dot(matrix.T, matrix, precision=lax.Precision.HIGHEST)
    factor_low = jnp.linalg.cholesky(gram_matrix)
    return lax.linalg.triangular_solve(factor_low, matrix, left_side=False, lower=True, transpose_a=True)

def reference(hidden, grad_out, weight_band, error_feedback, q_start):
    group_tokens = TOK_DEV * N_SHARD
    grad_scale = 1.0 / math.sqrt(TOK_DEV * N_SHARD * N_REP)
    d_hidden = lax.dot_general(grad_out.astype(jnp.float32), weight_band.astype(jnp.float32), (((1,), (1,)), ((), ())), preferred_element_type=jnp.float32).astype(jnp.bfloat16)
    hidden_groups = hidden.reshape(N_REP, group_tokens, BUCKET)
    out_groups = grad_out.reshape(N_REP, group_tokens, D)

    def group_grad(operands):
        return lax.dot_general(operands[0].astype(jnp.float32), operands[1].astype(jnp.float32), (((0,), (0,)), ((), ())), preferred_element_type=jnp.float32) * grad_scale
    grads = lax.map(group_grad, (hidden_groups, out_groups))
    merged = grads + error_feedback
    summed = lax.optimization_barrier(jnp.sum(merged, axis=0))
    q_factor = q_start
    p_factor = None
    for round_index in range(POWER):
        q_hat = orthonormal(q_factor)
        p_factor = orthonormal(jnp.dot(summed, q_hat, precision=lax.Precision.HIGHEST))
        q_factor = jnp.dot(summed.T, p_factor, precision=lax.Precision.HIGHEST)
    update = jnp.dot(p_factor, q_factor.T, precision=lax.Precision.HIGHEST)
    error_next = merged - update / N_REP
    return (update, error_next, q_factor, d_hidden)
```

```python
import functools
import math

import jax
import jax.numpy as jnp
from jax import lax
from jax.experimental import pallas as pl
from jax.experimental.pallas import tpu as pltpu
from jax.sharding import PartitionSpec as P

HIGHEST = lax.Precision.HIGHEST
NT = (((1,), (1,)), ((), ()))
NN = (((1,), (0,)), ((), ()))


def dot32(a, b, dims):
    return lax.dot_general(a, b, dims, precision=HIGHEST, preferred_element_type=jnp.float32)


def orth_rows(v):
    rank = v.shape[0]
    v = v * (1.0 / jnp.max(jnp.abs(v), axis=1, keepdims=True))
    rows = lax.broadcasted_iota(jnp.int32, (rank, 1), 0)
    for j in range(rank):
        pivot = v[j : j + 1, :]
        dots = jnp.sum(v * pivot, axis=1, keepdims=True)
        coef = jnp.where(rows > j, dots * (1.0 / dots[j : j + 1, :]), 0.0)
        v = v - coef * pivot
    return v * lax.rsqrt(jnp.sum(v * v, axis=1, keepdims=True))


def kernel(
    n_rep, n_shard, power, scale,
    h_ref, g_hbm, w_ref, ef_ref, q0_hbm,
    upd_ref, err_ref, qn_ref, dh_ref,
    gbuf, q0buf, part, oth, sib, rs, rep, mrow_s, mrow_r, wst, wsib, wa, qall, wall, wf,
    g_sem, q0_sem, d2d_s, d2d_r, rs_s, rs_r, rep_s, rep_r, mr_s, mr_r, ws_s, ws_r, wa_s, wa_r,
    q_s, q_r, qf_s, w_s, w_r, wfw_s,
):
    me = lax.axis_index("shard")
    my_rep = lax.axis_index("rep")
    n_chip = n_shard // 2
    chip = me // 2
    core = me % 2
    mate = chip * 2 + (1 - core)
    bucket = h_ref.shape[0]
    cols = rs.shape[2]
    own = ef_ref.shape[0]
    even = core == 0

    def chip_at(k):
        return lax.rem(chip + k, n_chip)

    def wide(c):
        return pl.ds(pl.multiple_of(c * (2 * cols), 2 * cols), 2 * cols)

    def remote(src, dst, ssem, rsem, **where):
        return pltpu.make_async_remote_copy(
            src_ref=src, dst_ref=dst, send_sem=ssem, recv_sem=rsem,
            device_id=where, device_id_type=pl.DeviceIdType.MESH,
        )

    order = list(range(n_chip - 1, 0, -1)) + [0]

    barrier = pltpu.get_barrier_semaphore()
    for k in range(1, n_shard):
        pl.semaphore_signal(
            barrier, inc=1, device_id={"shard": lax.rem(me + k, n_shard)},
            device_id_type=pl.DeviceIdType.MESH,
        )
    for k in range(1, n_rep):
        pl.semaphore_signal(
            barrier, inc=1, device_id={"rep": lax.rem(my_rep + k, n_rep)},
            device_id_type=pl.DeviceIdType.MESH,
        )

    def load(k):
        return pltpu.make_async_copy(g_hbm.at[:, wide(chip_at(k))], gbuf.at[k], g_sem.at[k])

    for k in order:
        load(k).start()
    q0_load = pltpu.make_async_copy(q0_hbm.at[:, wide(chip)], q0buf, q0_sem)
    q0_load.start()

    own_row = lax.broadcasted_iota(jnp.int32, (bucket, 1), 0) // own == me
    hidden = h_ref[...]

    def pair(k):
        return remote(oth.at[k], sib.at[k], d2d_s.at[k], d2d_r.at[k], shard=mate)

    for at, k in enumerate(order):
        load(k).wait()
        block = lax.dot_general(
            hidden, gbuf[k], NN, preferred_element_type=jnp.float32
        ) * scale
        error = jnp.concatenate([ef_ref[:, wide(chip_at(k))]] * n_shard, axis=0)
        block = block + jnp.where(own_row, error, 0.0)
        low, high = block[:, :cols], block[:, cols:]
        oth[k] = jnp.where(even, high, low)
        part[k] = jnp.where(even, low, high)
        if at == 0:
            pl.semaphore_wait(barrier, n_shard - 1 + n_rep - 1)
        pair(k).start()

    def scatter(k):
        return remote(
            part.at[k], rs.at[k], rs_s.at[k], rs_r.at[k], shard=chip_at(k) * 2 + core
        )

    for k in order:
        pair(k).wait_recv()
        part[k] = part[k] + sib[k]
        if k:
            scatter(k).start()
    merged = part[0]
    for k in order[:-1]:
        scatter(k).wait_recv()
        merged = merged + rs[k]
    rep[my_rep] = merged

    def across(k):
        other = lax.rem(my_rep + k, n_rep)
        return remote(
            rep.at[my_rep], rep.at[my_rep], rep_s.at[k], rep_r.at[k], rep=other
        )

    for k in range(1, n_rep):
        across(k).start()
    for s in range(n_shard):
        mrow_s[s] = merged[s * own : (s + 1) * own, :]
    mrow_r[me] = mrow_s[me]

    def row_send(k):
        to = lax.rem(me + k, n_shard)
        return remote(mrow_s.at[to], mrow_r.at[me], mr_s.at[k], mr_r.at[k], shard=to)

    for k in range(1, n_shard):
        row_send(k).start()
    for k in range(1, n_rep):
        across(k).wait_recv()
    summed = rep[0]
    for r in range(1, n_rep):
        summed = summed + rep[r]

    q0_load.wait()
    q_own = jnp.where(even, q0buf[:, :cols], q0buf[:, cols:])
    rank = q_own.shape[0]
    half = (bucket + rank) // 2
    term = dot32(jnp.concatenate([summed, q_own], axis=0), summed, NT)
    wst[...] = jnp.concatenate([term[:half], term[half:]], axis=1)
    mate_copy = remote(wst, wsib, ws_s.at[0], ws_r.at[0], shard=mate)
    mate_copy.start()
    mate_copy.wait_recv()
    wa[chip] = wst[...] + wsib[...]

    def term_send(k):
        return remote(
            wa.at[chip], wa.at[chip], wa_s.at[k], wa_r.at[k], shard=chip_at(k) * 2 + core
        )

    for k in order[:-1]:
        term_send(k).start()

    def w_send(k):
        to = mate if k == 0 else chip_at(k) * 2 + core
        return remote(w_ref, wall.at[me], w_s.at[k], w_r.at[k], shard=to)

    for k in order:
        w_send(k).start()
    wall[me] = w_ref[...]

    for k in order[:-1]:
        term_send(k).wait_recv()
    total = wa[0]
    for c in range(1, n_chip):
        total = total + wa[c]
    total = jnp.concatenate([total[:, :bucket], total[:, bucket:]], axis=0)
    square, y = total[:bucket], total[bucket:]
    p = orth_rows(y)
    for _ in range(power - 1):
        p = orth_rows(dot32(p, square, NN))

    qall[me] = dot32(p, summed, NN)

    def q_send(k):
        to = mate if k == 0 else chip_at(k) * 2 + core
        return remote(qall.at[me], qall.at[me], q_s.at[k], q_r.at[k], shard=to)

    for k in order:
        q_send(k).start()

    def source(k):
        return lax.rem(chip + n_chip - k, n_chip) * 2

    def w_pass(k):
        at = source(k) + core
        return remote(wall.at[at], wall.at[at], wfw_s.at[k], w_r.at[n_chip + k], shard=mate)

    def q_pass(k):
        at = source(k) + core
        return remote(qall.at[at], qall.at[at], qf_s.at[k], q_r.at[n_chip + k], shard=mate)

    for k in order[:-1]:
        w_send(k).wait_recv()
        w_pass(k).start()
    w_send(0).wait_recv()
    for k in order[:-1]:
        w_pass(k).wait_recv()
    for s in range(n_shard):
        wf[s * own : (s + 1) * own, :] = wall[s].astype(jnp.float32)
    dh = jnp.zeros(dh_ref.shape, jnp.float32)
    for k in range(n_chip):
        band = wf[:, wide(chip_at(k))].astype(jnp.bfloat16)
        dh = dh + lax.dot_general(band, gbuf[k], NT, preferred_element_type=jnp.float32)
    dh_ref[...] = dh.astype(jnp.bfloat16)

    for k in order[:-1]:
        q_send(k).wait_recv()
        q_pass(k).start()
    q_send(0).wait_recv()
    for k in order[:-1]:
        q_pass(k).wait_recv()
    for k in range(1, n_shard):
        row_send(k).wait_recv()

    pick = lax.broadcasted_iota(jnp.int32, (8, bucket), 1) == me * own + lax.broadcasted_iota(
        jnp.int32, (8, bucket), 0
    )
    p_own = dot32(pick.astype(jnp.float32), p, NT)
    for s in range(n_shard):
        here = slice(s * cols, (s + 1) * cols)
        q = qall[s]
        qn_ref[:, here] = q
        update = dot32(p_own, q, NN)[:own]
        upd_ref[:, here] = update
        err_ref[:, here] = mrow_r[s] - update * (1.0 / n_rep)

    for k in order:
        pair(k).wait_send()
        w_send(k).wait_send()
        q_send(k).wait_send()
        if k:
            scatter(k).wait_send()
            term_send(k).wait_send()
            w_pass(k).wait_send()
            q_pass(k).wait_send()
    mate_copy.wait_send()
    for k in range(1, n_rep):
        across(k).wait_send()
    for k in range(1, n_shard):
        row_send(k).wait_send()


POWER = 2


def body(n_rep, n_shard, hidden, grad_out, weight_band, error_feedback, q_start):
    tokens, bucket = hidden.shape
    width = grad_out.shape[1]
    own = weight_band.shape[0]
    rank = q_start.shape[1]
    cols = width // n_shard
    n_chip = n_shard // 2
    scale = 1.0 / math.sqrt(tokens * n_shard * n_rep)
    f32, bf16 = jnp.float32, jnp.bfloat16
    half = (bucket + rank) // 2
    dma = lambda *s: pltpu.SemaphoreType.DMA(s)
    vmem = pl.BlockSpec(memory_space=pltpu.VMEM)
    hbm = pl.BlockSpec(memory_space=pl.ANY)
    update, error, q_t, dh_t = pl.pallas_call(
        functools.partial(kernel, n_rep, n_shard, POWER, scale),
        out_shape=(
            jax.ShapeDtypeStruct((own, width), f32),
            jax.ShapeDtypeStruct((own, width), f32),
            jax.ShapeDtypeStruct((rank, width), f32),
            jax.ShapeDtypeStruct((bucket, tokens), bf16),
        ),
        in_specs=[vmem, hbm, vmem, vmem, hbm],
        out_specs=(vmem,) * 4,
        scratch_shapes=[
            pltpu.VMEM((n_chip, tokens, 2 * cols), bf16),
            pltpu.VMEM((rank, 2 * cols), f32),
            pltpu.VMEM((n_chip, bucket, cols), f32),
            pltpu.VMEM((n_chip, bucket, cols), f32),
            pltpu.VMEM((n_chip, bucket, cols), f32),
            pltpu.VMEM((n_chip, bucket, cols), f32),
            pltpu.VMEM((n_rep, bucket, cols), f32),
            pltpu.VMEM((n_shard, own, cols), f32),
            pltpu.VMEM((n_shard, own, cols), f32),
            pltpu.VMEM((half, 2 * bucket), f32),
            pltpu.VMEM((half, 2 * bucket), f32),
            pltpu.VMEM((n_chip, half, 2 * bucket), f32),
            pltpu.VMEM((n_shard, rank, cols), f32),
            pltpu.VMEM((n_shard, own, width), bf16),
            pltpu.VMEM((bucket, width), f32),
            dma(n_chip), dma(), dma(n_chip), dma(n_chip), dma(n_chip), dma(n_chip),
            dma(n_rep), dma(n_rep), dma(n_shard), dma(n_shard), dma(1), dma(1),
            dma(n_chip), dma(n_chip),
            dma(n_chip), dma(n_shard), dma(n_chip), dma(n_chip), dma(n_shard), dma(n_chip),
        ],
        compiler_params=pltpu.CompilerParams(
            collective_id=0, has_side_effects=True, vmem_limit_bytes=60 * 1024 * 1024
        ),
        name="bucket_step",
    )(hidden.T, grad_out, weight_band, error_feedback[0], q_start.T)
    return update, error[None], q_t.T, dh_t.T


def solution(mesh):
    return jax.shard_map(
        functools.partial(body, mesh.shape["rep"], mesh.shape["shard"]),
        mesh=mesh,
        in_specs=(
            P(("rep", "shard"), None),
            P(("rep", "shard"), None),
            P("shard", None),
            P("rep", "shard", None),
            P(),
        ),
        out_specs=(P("shard", None), P("rep", "shard", None), P(), P(("rep", "shard"), None)),
        check_vma=False,
    )
```

```python
import functools
import math

import jax
import jax.numpy as jnp
from jax import lax
from jax.experimental import pallas as pl
from jax.experimental.pallas import tpu as pltpu
from jax.sharding import PartitionSpec as P

HIGHEST = lax.Precision.HIGHEST
GROUP = 4
FINISH_LIMIT = 67043328
VMEM_LIMIT = 67043328
NT = (((1,), (1,)), ((), ()))
NN = (((1,), (0,)), ((), ()))


def dot32(a, b, dims):
    return lax.dot_general(a, b, dims, precision=HIGHEST, preferred_element_type=jnp.float32)


def orth_rows(v):
    rank = v.shape[0]
    v = v * (1.0 / jnp.max(jnp.abs(v), axis=1, keepdims=True))
    rows = lax.broadcasted_iota(jnp.int32, (rank, 1), 0)
    for first in range(0, rank, GROUP):
        pivots, dots, invs = [], [], []
        raw = [v[first + i : first + i + 1, :] for i in range(GROUP)]
        sums = [jnp.sum(v * pivot, axis=1, keepdims=True) for pivot in raw]
        for i in range(GROUP):
            at = first + i
            pivot, dot = raw[i], sums[i]
            for other, done, inv in zip(pivots, dots, invs):
                part = done[at : at + 1, :] * inv
                pivot = pivot - part * other
                dot = dot - part * done
            pivots.append(pivot)
            dots.append(dot)
            invs.append(1.0 / dot[at : at + 1, :])
        for i in range(GROUP):
            v = v - jnp.where(rows > first + i, dots[i] * invs[i], 0.0) * pivots[i]
    return v * lax.rsqrt(jnp.sum(v * v, axis=1, keepdims=True))


def kernel(
    n_rep, n_shard, power, scale,
    h_hbm, g_hbm, w_hbm, ef_hbm, q0_hbm,
    q_out, p_out, row_out, dh_out,
    h_ref, w_ref, ef_ref, p_ref, dh_ref, gbuf, q0buf, part, oth, sib, rs, rep, mrow_s, mrow_r, wst, wsib, wa, qall, wall, wf,
    g_sem, q0_sem, d2d_s, d2d_r, rs_s, rs_r, rep_s, rep_r, mr_s, mr_r, ws_s, ws_r, wa_s, wa_r,
    q_s, q_r, qf_s, w_s, w_r, wfw_s, in_sem, out_sem, qo_sem,
):
    me = lax.axis_index("shard")
    my_rep = lax.axis_index("rep")
    n_chip = n_shard // 2
    chip = me // 2
    core = me % 2
    mate = chip * 2 + (1 - core)
    bucket = h_ref.shape[0]
    cols = rs.shape[2]
    own = ef_ref.shape[0]
    even = core == 0

    def chip_at(k):
        return lax.rem(chip + k, n_chip)

    def wide(c):
        return pl.ds(pl.multiple_of(c * (2 * cols), 2 * cols), 2 * cols)

    def remote(src, dst, ssem, rsem, **where):
        return pltpu.make_async_remote_copy(
            src_ref=src, dst_ref=dst, send_sem=ssem, recv_sem=rsem,
            device_id=where, device_id_type=pl.DeviceIdType.MESH,
        )

    order = list(range(n_chip - 1, 0, -1)) + [0]

    barrier = pltpu.get_barrier_semaphore()
    for k in range(1, n_shard):
        pl.semaphore_signal(
            barrier, inc=1, device_id={"shard": lax.rem(me + k, n_shard)},
            device_id_type=pl.DeviceIdType.MESH,
        )
    for k in range(1, n_rep):
        pl.semaphore_signal(
            barrier, inc=1, device_id={"rep": lax.rem(my_rep + k, n_rep)},
            device_id_type=pl.DeviceIdType.MESH,
        )

    ins = [
        pltpu.make_async_copy(src, dst, in_sem.at[i])
        for i, (src, dst) in enumerate(((h_hbm, h_ref), (ef_hbm, ef_ref), (w_hbm, w_ref)))
    ]
    ins[0].start()
    ins[1].start()

    def load(k):
        return pltpu.make_async_copy(g_hbm.at[:, wide(chip_at(k))], gbuf.at[k], g_sem.at[k])

    for k in order:
        load(k).start()
    q0_load = pltpu.make_async_copy(q0_hbm.at[:, wide(chip)], q0buf, q0_sem)
    q0_load.start()
    ins[2].start()

    own_row = lax.broadcasted_iota(jnp.int32, (bucket, 1), 0) // own == me
    ins[0].wait()
    hidden = h_ref[...]
    ins[1].wait()

    def pair(k):
        return remote(oth.at[k], sib.at[k], d2d_s.at[k], d2d_r.at[k], shard=mate)

    for at, k in enumerate(order):
        load(k).wait()
        block = lax.dot_general(
            hidden, gbuf[k], NN, preferred_element_type=jnp.float32
        ) * scale
        error = jnp.concatenate([ef_ref[:, wide(chip_at(k))]] * n_shard, axis=0)
        block = block + jnp.where(own_row, error, 0.0)
        low, high = block[:, :cols], block[:, cols:]
        oth[k] = jnp.where(even, high, low)
        part[k] = jnp.where(even, low, high)
        if at == 0:
            pl.semaphore_wait(barrier, n_shard - 1 + n_rep - 1)
        pair(k).start()

    def scatter(k):
        return remote(
            part.at[k], rs.at[k], rs_s.at[k], rs_r.at[k], shard=chip_at(k) * 2 + core
        )

    for k in order:
        pair(k).wait_recv()
        part[k] = part[k] + sib[k]
        if k:
            scatter(k).start()
    merged = part[0]
    for k in order[:-1]:
        scatter(k).wait_recv()
        merged = merged + rs[k]
    rep[my_rep] = merged

    def across(k):
        other = lax.rem(my_rep + k, n_rep)
        return remote(
            rep.at[my_rep], rep.at[my_rep], rep_s.at[k], rep_r.at[k], rep=other
        )

    for k in range(1, n_rep):
        across(k).start()
    for s in range(n_shard):
        mrow_s[s] = merged[s * own : (s + 1) * own, :]
    mrow_r[me] = mrow_s[me]

    def row_send(k):
        to = lax.rem(me + k, n_shard)
        return remote(mrow_s.at[to], mrow_r.at[me], mr_s.at[k], mr_r.at[k], shard=to)

    for k in range(1, n_shard):
        row_send(k).start()
    for k in range(1, n_rep):
        across(k).wait_recv()
    summed = rep[0]
    for r in range(1, n_rep):
        summed = summed + rep[r]

    q0_load.wait()
    q_own = jnp.where(even, q0buf[:, :cols], q0buf[:, cols:])
    rank = q_own.shape[0]
    half = (bucket + rank) // 2
    term = dot32(jnp.concatenate([summed, q_own], axis=0), summed, NT)
    wst[...] = jnp.concatenate([term[:half], term[half:]], axis=1)
    mate_copy = remote(wst, wsib, ws_s.at[0], ws_r.at[0], shard=mate)
    mate_copy.start()
    mate_copy.wait_recv()
    wa[chip] = wst[...] + wsib[...]

    def term_send(k):
        return remote(
            wa.at[chip], wa.at[chip], wa_s.at[k], wa_r.at[k], shard=chip_at(k) * 2 + core
        )

    for k in order[:-1]:
        term_send(k).start()

    def w_send(k):
        to = mate if k == 0 else chip_at(k) * 2 + core
        return remote(w_ref, wall.at[me], w_s.at[k], w_r.at[k], shard=to)

    ins[2].wait()
    for k in order:
        w_send(k).start()
    wall[me] = w_ref[...]

    for k in order[:-1]:
        term_send(k).wait_recv()
    total = wa[0]
    for c in range(1, n_chip):
        total = total + wa[c]
    total = jnp.concatenate([total[:, :bucket], total[:, bucket:]], axis=0)
    square, y = total[:bucket], total[bucket:]
    p = orth_rows(y)
    for _ in range(power - 1):
        p = orth_rows(dot32(p, square, NN))

    qall[me] = dot32(p, summed, NN)

    def q_send(k):
        to = mate if k == 0 else chip_at(k) * 2 + core
        return remote(qall.at[me], qall.at[me], q_s.at[k], q_r.at[k], shard=to)

    for k in order:
        q_send(k).start()

    def source(k):
        return lax.rem(chip + n_chip - k, n_chip) * 2

    def w_pass(k):
        at = source(k) + core
        return remote(wall.at[at], wall.at[at], wfw_s.at[k], w_r.at[n_chip + k], shard=mate)

    def q_pass(k):
        at = source(k) + core
        return remote(qall.at[at], qall.at[at], qf_s.at[k], q_r.at[n_chip + k], shard=mate)

    for k in order[:-1]:
        w_send(k).wait_recv()
        w_pass(k).start()
    w_send(0).wait_recv()
    for k in order[:-1]:
        w_pass(k).wait_recv()
    for s in range(n_shard):
        wf[s * own : (s + 1) * own, :] = wall[s].astype(jnp.float32)
    dh = jnp.zeros(dh_ref.shape, jnp.float32)
    for k in range(n_chip):
        band = wf[:, wide(chip_at(k))].astype(jnp.bfloat16)
        dh = dh + lax.dot_general(band, gbuf[k], NT, preferred_element_type=jnp.float32)
    dh_ref[...] = dh.astype(jnp.bfloat16)

    outs = [
        pltpu.make_async_copy(src, dst, out_sem.at[i])
        for i, (src, dst) in enumerate(((dh_ref, dh_out), (p_ref, p_out), (mrow_r, row_out)))
    ]
    outs[0].start()
    pick = lax.broadcasted_iota(jnp.int32, (8, bucket), 1) == me * own + lax.broadcasted_iota(
        jnp.int32, (8, bucket), 0
    )
    p_ref[...] = dot32(pick.astype(jnp.float32), p, NT)
    outs[1].start()
    for k in range(1, n_shard):
        row_send(k).wait_recv()
    outs[2].start()

    def q_write(k, mine):
        at = source(k) + (core if mine else 1 - core)
        return pltpu.make_async_copy(
            qall.at[at], q_out.at[at], qo_sem.at[k if mine else n_chip + k]
        )

    q_write(0, True).start()
    for k in order[:-1]:
        q_send(k).wait_recv()
        q_pass(k).start()
        q_write(k, True).start()
    q_send(0).wait_recv()
    q_write(0, False).start()
    for k in order[:-1]:
        q_pass(k).wait_recv()
        q_write(k, False).start()

    for k in order:
        pair(k).wait_send()
        w_send(k).wait_send()
        q_send(k).wait_send()
        if k:
            scatter(k).wait_send()
            term_send(k).wait_send()
            w_pass(k).wait_send()
            q_pass(k).wait_send()
    mate_copy.wait_send()
    for k in range(1, n_rep):
        across(k).wait_send()
    for k in range(1, n_shard):
        row_send(k).wait_send()

    for copy in outs:
        copy.wait()
    for k in range(n_chip):
        q_write(k, True).wait()
        q_write(k, False).wait()


def finish(
    n_rep, n_shard, q_in, p_in, row_in, dh_in,
    upd_out, err_out, qn_out, dh_out, q_ref, p_ref, row_ref, upd, err, qn, sems, dh_sem, in_sem,
):
    own, cols = row_ref.shape[1:]
    ins = [
        pltpu.make_async_copy(src, dst, in_sem.at[i])
        for i, (src, dst) in enumerate(((p_in, p_ref), (row_in, row_ref), (q_in, q_ref)))
    ]
    for copy in ins:
        copy.start()
    dh_copy = pltpu.make_async_copy(dh_in, dh_out, dh_sem)
    dh_copy.start()
    for copy in ins:
        copy.wait()
    p_own = p_ref[...]
    copies = []
    for c in range(n_shard // 2):
        here = slice(c * 2 * cols, (c + 1) * 2 * cols)
        q = jnp.concatenate([q_ref[2 * c], q_ref[2 * c + 1]], axis=1)
        rows = jnp.concatenate([row_ref[2 * c], row_ref[2 * c + 1]], axis=1)
        qn[:, here] = q
        update = dot32(p_own, q, NN)[:own]
        upd[:, here] = update
        err[:, here] = rows - update * (1.0 / n_rep)
        for i, (src, dst) in enumerate(((upd, upd_out), (err, err_out), (qn, qn_out))):
            copies.append(pltpu.make_async_copy(src.at[:, here], dst.at[:, here], sems.at[i, c]))
            copies[-1].start()
    for copy in copies:
        copy.wait()
    dh_copy.wait()


POWER = 2


def body(n_rep, n_shard, hidden, grad_out, weight_band, error_feedback, q_start):
    tokens, bucket = hidden.shape
    width = grad_out.shape[1]
    own = weight_band.shape[0]
    rank = q_start.shape[1]
    cols = width // n_shard
    n_chip = n_shard // 2
    scale = 1.0 / math.sqrt(tokens * n_shard * n_rep)
    f32, bf16 = jnp.float32, jnp.bfloat16
    half = (bucket + rank) // 2
    dma = lambda *s: pltpu.SemaphoreType.DMA(s)
    hbm = pl.BlockSpec(memory_space=pl.ANY)
    q3, p_own, rows, dh = pl.pallas_call(
        functools.partial(kernel, n_rep, n_shard, POWER, scale),
        out_shape=(
            jax.ShapeDtypeStruct((n_shard, rank, cols), f32),
            jax.ShapeDtypeStruct((8, rank), f32),
            jax.ShapeDtypeStruct((n_shard, own, cols), f32),
            jax.ShapeDtypeStruct((bucket, tokens), bf16),
        ),
        in_specs=[pl.BlockSpec(memory_space=pltpu.HBM)] * 5,
        out_specs=(hbm,) * 4,
        scratch_shapes=[
            pltpu.VMEM((bucket, tokens), bf16),
            pltpu.VMEM((own, width), bf16),
            pltpu.VMEM((own, width), f32),
            pltpu.VMEM((8, rank), f32),
            pltpu.VMEM((bucket, tokens), bf16),
            pltpu.VMEM((n_chip, tokens, 2 * cols), bf16),
            pltpu.VMEM((rank, 2 * cols), f32),
            pltpu.VMEM((n_chip, bucket, cols), f32),
            pltpu.VMEM((n_chip, bucket, cols), f32),
            pltpu.VMEM((n_chip, bucket, cols), f32),
            pltpu.VMEM((n_chip, bucket, cols), f32),
            pltpu.VMEM((n_rep, bucket, cols), f32),
            pltpu.VMEM((n_shard, own, cols), f32),
            pltpu.VMEM((n_shard, own, cols), f32),
            pltpu.VMEM((half, 2 * bucket), f32),
            pltpu.VMEM((half, 2 * bucket), f32),
            pltpu.VMEM((n_chip, half, 2 * bucket), f32),
            pltpu.VMEM((n_shard, rank, cols), f32),
            pltpu.VMEM((n_shard, own, width), bf16),
            pltpu.VMEM((bucket, width), f32),
            dma(n_chip), dma(), dma(n_chip), dma(n_chip), dma(n_chip), dma(n_chip),
            dma(n_rep), dma(n_rep), dma(n_shard), dma(n_shard), dma(1), dma(1),
            dma(n_chip), dma(n_chip),
            dma(n_chip), dma(n_shard), dma(n_chip), dma(n_chip), dma(n_shard), dma(n_chip),
            dma(3), dma(3), dma(n_shard),
        ],
        compiler_params=pltpu.CompilerParams(
            collective_id=0, has_side_effects=True, vmem_limit_bytes=VMEM_LIMIT
        ),
        name="bucket_step",
    )(hidden.T, grad_out, weight_band, error_feedback[0], q_start.T)
    update, error, q_t, dh_t = pl.pallas_call(
        functools.partial(finish, n_rep, n_shard),
        out_shape=(
            jax.ShapeDtypeStruct((own, width), f32),
            jax.ShapeDtypeStruct((own, width), f32),
            jax.ShapeDtypeStruct((rank, width), f32),
            jax.ShapeDtypeStruct((bucket, tokens), bf16),
        ),
        in_specs=[hbm] * 4,
        out_specs=(pl.BlockSpec(memory_space=pltpu.HBM),) * 4,
        scratch_shapes=[
            pltpu.VMEM((n_shard, rank, cols), f32),
            pltpu.VMEM((8, rank), f32),
            pltpu.VMEM((n_shard, own, cols), f32),
            pltpu.VMEM((own, width), f32),
            pltpu.VMEM((own, width), f32),
            pltpu.VMEM((rank, width), f32),
            dma(3, n_chip), dma(), dma(3),
        ],
        compiler_params=pltpu.CompilerParams(vmem_limit_bytes=FINISH_LIMIT),
        name="outputs",
    )(q3, p_own, rows, dh)
    return update, error[None], q_t.T, dh_t.T


def solution(mesh):
    return jax.shard_map(
        functools.partial(body, mesh.shape["rep"], mesh.shape["shard"]),
        mesh=mesh,
        in_specs=(
            P(("rep", "shard"), None),
            P(("rep", "shard"), None),
            P("shard", None),
            P("rep", "shard", None),
            P(),
        ),
        out_specs=(P("shard", None), P("rep", "shard", None), P(), P(("rep", "shard"), None)),
        check_vma=False,
    )
```
